32 devices in a mesh: row: 8 (over z, core), col: 4 (over y, x).
Axes of the slice: x: 2, y: 2, z: 4, core: 2. Of those that a mesh axis runs over, the one named last changes fastest.
Arguments:
- matrix: bfloat16 [4096, 4096], P('row', 'col'), may hold values from -6 to 6
- factors: float32 [4096, 4096], P('row', 'col')
- inverse: bfloat16 [32, 128, 128], P('col'), may hold values from -0.007171631 to 0.007171631
- pattern: int32 [32, 32], P('row', 'col'), may hold values from 0 to 1, as said below
- dropped: int32 [32, 32], P('row', 'col'), may hold values from 0 to 1, as said below
Outputs:
- factors_out: float32 [4096, 4096], P('row', 'col')
The draws below stay inside these ranges and needn't reach their ends.
Inputs may be any that keep to these rules, and one draw needn't show every extreme that they name: Block (I, J) can be in the pattern only where I - J is 0, 1, -1, 4, -4, 16 or -16; the blocks with I - J of 0, 1, -1, 4 and -4 are always in it. In each device's region of 4 block rows by 8 block columns, every block column holds at most 3 pattern blocks (exactly 3 in some columns), and every block row at most 2 pattern blocks below the block diagonal (exactly 2 in some rows). `dropped`: dropped blocks lie in the pattern and off the block diagonal.
All inputs are finite; a program needn't handle non-finite values.
Results may differ from the reference program's by a relative error of at most 0.00083.
Values may be sent and summed in bfloat16 or wider, within the bound.
A program may use at most 128 MiB of HBM per device.

```python
import jax
import jax.numpy as jnp
from jax import lax

BS = 128
RB = 4
SWEEPS = 2
NB = 32
N = 4096


def pattern_from(key):
    row_number = jnp.arange(NB)[:, None]
    col_number = jnp.arange(NB)[None, :]
    offset = jnp.abs(row_number - col_number)
    band = (offset <= 1) | (offset == RB)
    far = offset == NB // 2
    lowest = jnp.minimum(row_number, col_number)
    coin_vector = jax.random.randint(jax.random.fold_in(key, 11), (NB,), 0, 2)
    keep_far = (coin_vector[lowest] == 1) | (lowest % RB == 0)
    return (band | far & keep_far).astype(jnp.int32)


def draw_pattern(key, part):
    return pattern_from(key)


def draw_dropped(key, part):
    member = pattern_from(key)
    coin = jax.random.randint(jax.random.fold_in(key, 13), (NB, NB), 0, 4) == 0
    row_number = jnp.arange(NB)[:, None]
    col_number = jnp.arange(NB)[None, :]
    off_diagonal = row_number != col_number
    return (member * coin * off_diagonal).astype(jnp.int32)


def draw_factors(key, part):
    block_number = jnp.arange(N) // BS
    below = block_number[:, None] > block_number[None, :]
    spread = jnp.where(below, 0.015, 1.0).astype(jnp.float32)
    raw_values = jax.random.normal(key, (N, N), jnp.float32)
    return (raw_values * spread).astype(jnp.float32)


def block_levels(rng, extent, split, smallest, high):
    factor_of, own = 1.0, jax.random.fold_in(rng, 6)
    for axis_at, blocks in split:
        steps = jnp.exp(jax.random.uniform(jax.random.fold_in(own, axis_at), (blocks,), jnp.float32, smallest / len(split), high / len(split)))
        factor_of = factor_of * jnp.repeat(steps, extent[axis_at] // blocks).reshape([-1 if axis == axis_at else 1 for axis in range(len(extent))])
    return factor_of


def normal_values(own_key, extent, width, bound, split=(), kind=jnp.bfloat16):
    level = block_levels(own_key, extent, split, -0.22, 0.18) if split else 1.0
    entries = jax.random.normal(own_key, extent, jnp.float32) * width * level
    return jnp.minimum(jnp.maximum(entries, -bound), bound).astype(kind)


def setup_inputs(seed: int = 0) -> dict:
    streams_of = jax.random.split(jax.random.key(seed), 6)
    matrix = normal_values(streams_of[0], (N, N), 1.0, 6.0, ((0, 8), (1, 4)))
    factors = draw_factors(jax.random.fold_in(streams_of[5], 71), 0)
    inverse = normal_values(streams_of[2], (NB, BS, BS), 0.0012, 0.007171631, ((0, 4),))
    pattern = draw_pattern(jax.random.fold_in(streams_of[5], 71), 0)
    dropped = draw_dropped(jax.random.fold_in(streams_of[5], 71), 0)
    return {"matrix": matrix, "factors": factors, "inverse": inverse, "pattern": pattern, "dropped": dropped}


def expand(block_mask):
    return jnp.repeat(jnp.repeat(block_mask, BS, axis=0), BS, axis=1)


def reference(matrix, factors, inverse, pattern, dropped):
    row_number = jnp.arange(NB)[:, None]
    col_number = jnp.arange(NB)[None, :]
    member = pattern == 1
    lower_mask = expand((member & (row_number > col_number)).astype(jnp.float32))
    upper_mask = expand((member & (row_number <= col_number)).astype(jnp.float32))
    in_pattern = expand(member.astype(jnp.float32))
    low_part = factors * lower_mask
    up_part = factors * upper_mask
    dense_matrix = matrix.astype(jnp.float32)
    inverse_full = inverse.astype(jnp.float32)
    for sweep_index in range(SWEEPS):
        low_half = lax.optimization_barrier(low_part.astype(jnp.bfloat16)).astype(jnp.float32)
        up_half = lax.optimization_barrier(up_part.astype(jnp.bfloat16)).astype(jnp.float32)
        product = jnp.dot(low_half, up_half, precision=lax.Precision.HIGHEST)
        residual = (dense_matrix - product - up_part) * in_pattern
        rounded = lax.optimization_barrier(residual.astype(jnp.bfloat16)).astype(jnp.float32)
        rounded = rounded.reshape(N, NB, BS)
        correction = jnp.einsum("rjb,jbc->rjc", rounded, inverse_full, precision=lax.Precision.HIGHEST)
        low_part = low_part + correction.reshape(N, N) * lower_mask
        up_part = up_part + residual * upper_mask
    keep_mask = expand((1 - dropped).astype(jnp.float32))
    return (low_part + up_part) * keep_mask
```

```python
import functools

import jax
import jax.numpy as jnp
from jax import lax
from jax.experimental import pallas as pl
from jax.experimental.pallas import tpu as pltpu
from jax.sharding import PartitionSpec as P

SWEEPS = 2
MESH = pl.DeviceIdType.MESH
F32 = jnp.float32
BF16 = jnp.bfloat16

SLOTS = 4
DIAG, LEFT, RIGHT, OUTER = range(SLOTS)
D_NEAR, D_FAR, L_NEAR, U_NEAR, L_FAR, U_FAR = range(6)


def dot(x, y):
    return jnp.dot(x, y, preferred_element_type=F32)


def sweep_kernel(
    rows, cols, row_devices, col_devices, bs,
    pattern_in, dropped_in, matrix, factors, inverse_in, out,
    pattern, dropped, flag_sem, a, inverse, lb, ub, sd, rd, rln, run, rlf, ruf, acc,
    load_sem, inverse_sem, send_sem, recv_sem,
):
    r, c = lax.axis_index("row"), lax.axis_index("col")
    far_r, far_c = row_devices // 2, col_devices // 2
    q = r - (cols // rows) * c
    barrier = pltpu.get_barrier_semaphore()

    def loads(i, s, j):
        k = i * SLOTS + s
        src = (pl.ds(i * bs, bs), pl.ds(pl.multiple_of(j * bs, bs), bs))
        return (
            pltpu.make_async_copy(factors.at[src], out.at[k], load_sem.at[0, k]),
            pltpu.make_async_copy(matrix.at[src], a.at[k], load_sem.at[1, k]),
        )

    def start_loads(blocks):
        for block in blocks:
            for copy in loads(*block):
                copy.start()

    def wait_loads(blocks):
        for block in blocks:
            for copy in loads(*block):
                copy.wait()

    flag_copies = (
        pltpu.make_async_copy(pattern_in, pattern, flag_sem.at[0]),
        pltpu.make_async_copy(dropped_in, dropped, flag_sem.at[1]),
    )
    for copy in flag_copies:
        copy.start()
    inverse_copy = pltpu.make_async_copy(inverse_in, inverse, inverse_sem)

    def hello(r2, c2):
        pl.semaphore_signal(barrier, inc=1, device_id=(r2, c2), device_id_type=MESH)

    def message(kind, v, src, dst, slot, r2, c2):
        return pltpu.make_async_remote_copy(
            src_ref=src, dst_ref=dst,
            send_sem=send_sem.at[kind, v], recv_sem=recv_sem.at[slot, v],
            device_id=(r2, c2), device_id_type=MESH,
        )

    def d_near(v):
        return message(D_NEAR, v, sd.at[v], rd.at[v], D_NEAR, r + 1, c)

    def d_far(v):
        return message(D_FAR, v, sd.at[v], rd.at[v], D_NEAR, r + far_r, c)

    def l_near(v):
        return message(L_NEAR, v, lb.at[v, pl.ds(0, rows + 1)], rln.at[v], L_NEAR, r, c + 1)

    def u_near(v):
        return message(U_NEAR, v, ub.at[v, pl.ds(0, rows + 1)], run.at[v], U_NEAR, r + 1, c)

    def l_far(v):
        return message(L_FAR, v, lb.at[v, pl.ds(0, rows)], rlf.at[v], L_FAR, r, c + far_c)

    def u_far(v):
        return message(U_FAR, v, ub.at[v, pl.ds(0, rows)], ruf.at[v], U_FAR, r + far_r, c)

    def lower_step(k, b, v, diag, j, mask=None):
        product = dot(lb[v, b], diag)
        residual = a[k].astype(F32) - product
        if mask is not None:
            residual = residual * mask
        correction = dot(residual.astype(BF16), inverse[j])
        if mask is not None:
            correction = correction * mask
        out[k] = out[k] + correction
        if v + 1 < SWEEPS:
            lb[v + 1, b] = out[k].astype(BF16)

    def upper_steps(k, b, mask=None):
        for v in range(SWEEPS):
            ub[v, b] = out[k].astype(BF16)
            residual = a[k].astype(F32) - out[k]
            if mask is not None:
                residual = residual * mask
            out[k] = out[k] + residual

    def wait_flag(n):
        flag_copies[n].wait()

    def keep(i, s, j):
        k = i * SLOTS + s
        out[k] = out[k] * (1 - dropped[i, j]).astype(F32)

    out[rows * SLOTS] = jnp.zeros((bs, bs), F32)

    def diagonal_owner(h):
        base = h * rows
        below = [(i, LEFT, base + i - 1) for i in range(rows) if base + i >= 1]
        right = [(i, RIGHT, base + i + 1) for i in range(rows) if base + i + 1 < cols]
        diag = [(i, DIAG, base + i) for i in range(rows)]
        outer = [(i, OUTER, i if h else rows + i) for i in range(rows)]
        has_far = c >= far_c
        sends_far = c < far_c
        has_near = c >= 1
        sends_near = c + 1 < col_devices

        def when_near_in(f):
            if h:
                f()
            else:
                pl.when(has_near)(f)

        def when_near_out(f):
            if h:
                pl.when(sends_near)(f)
            else:
                f()

        start_loads(diag)
        start_loads(outer)
        start_loads(right)
        start_loads(below)
        inverse_copy.start()

        def hello_near():
            hello(r - 1, c)
            if not h:
                hello(r, c - 1)

        when_near_in(hello_near)

        @pl.when(has_far)
        def _():
            hello(r - far_r, c)
            hello(r, c - far_c)

        wait_loads(diag)
        for i in range(rows):
            sd[0, i] = out[i * SLOTS + DIAG].astype(BF16)
        near_peers = sends_near.astype(jnp.int32) if h else 1
        peers = near_peers + sends_far.astype(jnp.int32)
        pl.when(peers > 0)(lambda: pl.semaphore_wait(barrier, peers))

        def send_d(v):
            pl.when(sends_far)(lambda: d_far(v).start())
            when_near_out(lambda: d_near(v).start())

        send_d(0)
        wait_loads(outer)
        wait_loads(right)
        for i, s, j in right:
            upper_steps(i * SLOTS + s, 2 * rows - 1 - i)
        if not h:
            for i, s, j in outer:
                upper_steps(i * SLOTS + s, i)
            u_near(0).start()
            u_near(1).start()
        wait_loads(below)
        for i, s, j in below:
            lb[0, rows + i] = out[i * SLOTS + s].astype(BF16)
        if h:
            for i, s, j in outer:
                lb[0, i] = out[i * SLOTS + s].astype(BF16)
        inverse_copy.wait()

        for v in range(SWEEPS):
            acc[0] = jnp.zeros((bs, bs), F32)
            for i in range(1, rows):
                acc[i] = dot(lb[v, rows + i], ub[v, 2 * rows - i])

            def near_terms():
                u_near_in = message(U_NEAR, v, ub.at[v, pl.ds(0, rows + 1)], run.at[v], U_NEAR, r - 1, c)
                u_near_in.wait_recv()
                if h:
                    left = lb
                else:
                    message(L_NEAR, v, lb.at[v, pl.ds(0, rows + 1)], rln.at[v], L_NEAR, r, c - 1).wait_recv()
                    left = rln
                acc[0] = acc[0] + dot(left[v, rows], run[v, rows])
                for i in range(rows):
                    acc[i] = acc[i] + dot(left[v, i], run[v, i])

            def far_terms():
                message(U_FAR, v, ub.at[v, pl.ds(0, rows)], ruf.at[v], U_FAR, r - far_r, c).wait_recv()
                message(L_FAR, v, lb.at[v, pl.ds(0, rows)], rlf.at[v], L_FAR, r, c - far_c).wait_recv()
                for i in range(rows):
                    acc[i] = acc[i] + dot(rlf[v, i], ruf[v, i])

            def local_lower():
                for i in range(1, rows):
                    lower_step(i * SLOTS + LEFT, rows + i, v, sd[v, i - 1], base + i - 1)

            def lower_from_before():
                if h:
                    message(D_NEAR, v, sd.at[v], rd.at[v], D_NEAR, r - 1, c).wait_recv()
                    lower_step(LEFT, rows, v, rd[v, rows - 1], rows - 1)
                    for i in range(rows):
                        lower_step(i * SLOTS + OUTER, i, v, rd[v, i], i)

            def diag_step():
                for i in range(rows):
                    k = i * SLOTS + DIAG
                    residual = a[k].astype(F32) - acc[i] - out[k]
                    out[k] = out[k] + residual
                    if v + 1 < SWEEPS:
                        sd[v + 1, i] = out[k].astype(BF16)
                if v + 1 < SWEEPS:
                    send_d(v + 1)

            local_lower()
            when_near_in(near_terms)
            if v + 1 < SWEEPS:
                pl.when(has_far)(far_terms)
                diag_step()
                lower_from_before()
            else:
                lower_from_before()
                pl.when(has_far)(far_terms)
                diag_step()

        wait_flag(0)
        wait_flag(1)
        for i, s, j in below + right + outer:
            keep(i, s, j)
        for v in range(SWEEPS):
            when_near_out(lambda: d_near(v).wait_send())
            pl.when(sends_far)(lambda: d_far(v).wait_send())
            if not h:
                u_near(v).wait_send()

    def lower_owner(blocks, source_r, l_message, far):
        places = [(i, s, j) for i, s, j, b, n in blocks]
        start_loads(places)
        inverse_copy.start()
        hello(source_r, c)
        wait_loads(places)
        wait_flag(0)
        masks = {}
        for i, s, j, b, n in blocks:
            k = i * SLOTS + s
            masks[k] = pattern[i, j].astype(F32) if far else None
            if far:
                out[k] = out[k] * masks[k]
            lb[0, b] = out[k].astype(BF16)
        pl.semaphore_wait(barrier, 1)
        l_message(0).start()
        inverse_copy.wait()
        for v in range(SWEEPS):
            message(D_NEAR, v, sd.at[v], rd.at[v], D_NEAR, source_r, c).wait_recv()
            for i, s, j, b, n in blocks:
                k = i * SLOTS + s
                lower_step(k, b, v, rd[v, n], j, masks[k])
            if v + 1 < SWEEPS:
                l_message(v + 1).start()
        wait_flag(1)
        for i, s, j in places:
            keep(i, s, j)
        for v in range(SWEEPS):
            l_message(v).wait_send()

    def upper_owner(blocks, u_message, far):
        places = [(i, s, j) for i, s, j, b in blocks]
        start_loads(places)
        wait_loads(places)
        wait_flag(0)
        for i, s, j, b in blocks:
            k = i * SLOTS + s
            mask = pattern[i, j].astype(F32) if far else None
            if far:
                out[k] = out[k] * mask
            upper_steps(k, b, mask)
        pl.semaphore_wait(barrier, 1)
        for v in range(SWEEPS):
            u_message(v).start()
        wait_flag(1)
        for i, s, j in places:
            keep(i, s, j)
        for v in range(SWEEPS):
            u_message(v).wait_send()

    far_roles = [q == k for f in (-far_r, far_r) for k in (f, f + 1)]
    idle = ~((q >= -1) & (q <= 2))
    for role in far_roles:
        idle = idle & ~role

    @pl.when(idle)
    def _():
        wait_flag(0)
        wait_flag(1)

    pl.when(q == 0)(lambda: diagonal_owner(0))
    pl.when(q == 1)(lambda: diagonal_owner(1))

    @pl.when(q == 2)
    def _():
        blocks = [(i, OUTER, rows + i, i, i) for i in range(rows)]
        lower_owner(blocks + [(0, LEFT, cols - 1, rows, rows - 1)], r - 1, l_near, False)

    @pl.when(q == -1)
    def _():
        blocks = [(i, OUTER, i, i) for i in range(rows)]
        upper_owner(blocks + [(rows - 1, RIGHT, 0, rows)], u_near, False)

    @pl.when((q == far_r) | (q == far_r + 1))
    def _():
        base = (q - far_r) * rows
        blocks = [(i, OUTER, base + i, i, i) for i in range(rows)]
        lower_owner(blocks, r - far_r, l_far, True)

    @pl.when((q == -far_r) | (q == 1 - far_r))
    def _():
        base = (q + far_r) * rows
        blocks = [(i, OUTER, base + i, i) for i in range(rows)]
        upper_owner(blocks, u_far, True)


def place_kernel(rows, cols, row_devices, bs, blocks, out, sem):
    r, c = lax.axis_index("row"), lax.axis_index("col")
    q = r - (cols // rows) * c
    far = (row_devices // 2) * rows
    copies = []
    for i in range(rows):
        for j in range(cols):
            d = rows * q + i - j
            k = jnp.where(
                d == 0, i * SLOTS + DIAG,
                jnp.where(
                    d == 1, i * SLOTS + LEFT,
                    jnp.where(
                        d == -1, i * SLOTS + RIGHT,
                        jnp.where(
                            (d == rows) | (d == -rows) | (d == far) | (d == -far),
                            i * SLOTS + OUTER, rows * SLOTS,
                        ),
                    ),
                ),
            )
            dst = out.at[pl.ds(i * bs, bs), pl.ds(j * bs, bs)]
            copies.append(pltpu.make_async_copy(blocks.at[k], dst, sem.at[i * cols + j]))
    for copy in copies:
        copy.start()
    for copy in copies:
        copy.wait()


def solution(mesh):
    row_devices, col_devices = mesh.shape["row"], mesh.shape["col"]

    def on_device(matrix, factors, inverse, pattern, dropped):
        rows, cols = pattern.shape
        bs = inverse.shape[1]
        places = rows * SLOTS
        half = lambda *n: pltpu.VMEM(n + (bs, bs), BF16)
        hbm = pl.BlockSpec(memory_space=pl.ANY)
        vmem = pl.BlockSpec(memory_space=pltpu.VMEM)
        blocks = pl.pallas_call(
            functools.partial(sweep_kernel, rows, cols, row_devices, col_devices, bs),
            out_shape=pltpu.VMEM((places + 1, bs, bs), F32),
            in_specs=[hbm] * 5,
            out_specs=vmem,
            scratch_shapes=[
                pltpu.SMEM((rows, cols), jnp.int32), pltpu.SMEM((rows, cols), jnp.int32),
                pltpu.SemaphoreType.DMA((2,)),
                half(places), half(cols), half(SWEEPS, 2 * rows), half(SWEEPS, 2 * rows),
                half(SWEEPS, rows), half(SWEEPS, rows),
                half(SWEEPS, rows + 1), half(SWEEPS, rows + 1), half(SWEEPS, rows), half(SWEEPS, rows),
                pltpu.VMEM((rows, bs, bs), F32),
                pltpu.SemaphoreType.DMA((2, places)),
                pltpu.SemaphoreType.DMA,
                pltpu.SemaphoreType.DMA((6, SWEEPS)),
                pltpu.SemaphoreType.DMA((6, SWEEPS)),
            ],
            compiler_params=pltpu.CompilerParams(collective_id=0, has_side_effects=True),
            name="sweeps",
        )(pattern, dropped, matrix, factors, inverse)
        return pl.pallas_call(
            functools.partial(place_kernel, rows, cols, row_devices, bs),
            out_shape=jax.ShapeDtypeStruct(factors.shape, F32),
            in_specs=[vmem],
            out_specs=hbm,
            scratch_shapes=[pltpu.SemaphoreType.DMA((rows * cols,))],
            name="place",
        )(pltpu.with_memory_space_constraint(blocks, pltpu.VMEM))

    placed = (P("row", "col"), P("row", "col"), P("col", None, None), P("row", "col"), P("row", "col"))
    return jax.shard_map(
        on_device, mesh=mesh, in_specs=placed, out_specs=P("row", "col"), check_vma=False
    )
```

```python
import functools

import jax
import jax.numpy as jnp
from jax import lax
from jax.experimental import pallas as pl
from jax.experimental.pallas import tpu as pltpu
from jax.sharding import PartitionSpec as P

SWEEPS = 2
MESH = pl.DeviceIdType.MESH
F32 = jnp.float32
BF16 = jnp.bfloat16

SLOTS = 4
DIAG, LEFT, RIGHT, OUTER = range(SLOTS)
D, L_NEAR, U_NEAR, L_FAR, U_FAR = range(5)

def dot(x, y):
    return jnp.dot(x, y, preferred_element_type=F32)


def sweep_kernel(
    rows, cols, row_devices, col_devices, bs,
    pattern_in, dropped_in, matrix, factors, inverse_in, out,
    pattern, dropped, a, inverse, lb, ub, sd, rd, rln, run, rlf, ruf, acc,
    flag_sem, load_sem, lead_sem, send_sem, recv_sem,
):
    r, c = lax.axis_index("row"), lax.axis_index("col")
    far_r, far_c = row_devices // 2, col_devices // 2
    last = col_devices - 1
    q = r - (cols // rows) * c
    barrier = pltpu.get_barrier_semaphore()
    inbox = {D: rd, L_NEAR: rln, U_NEAR: run, L_FAR: rlf, U_FAR: ruf}
    half = rows // 2

    near = [(0, 1 + half), (1 + half, rows - half)]
    far = [(0, half), (half, rows - half)]
    parts = {
        D: [(n, 1) for n in range(rows)], L_NEAR: [(n, 1) for n in range(rows + 1)],
        U_NEAR: near, L_FAR: far, U_FAR: far,
    }
    first_sem = {D: 0, L_NEAR: 0}
    for kind, before, size in ((U_NEAR, L_NEAR, rows + 1), (L_FAR, U_NEAR, 2), (U_FAR, L_FAR, 2)):
        first_sem[kind] = first_sem[before] + SWEEPS * size

    def arrival(kind, v, p):
        size = rows + 1 if kind in (D, L_NEAR) else 2
        return recv_sem.at[first_sem[kind] + v * size + p]

    def part_of(kind, n):
        return max(p for p, (start, size) in enumerate(parts[kind]) if start <= n)

    pending, seen = [], set()

    def remote(kind, v, p, buf, r2, c2):
        at = (v, pl.ds(*parts[kind][p]))
        return pltpu.make_async_remote_copy(
            src_ref=buf.at[at], dst_ref=inbox[kind].at[at],
            send_sem=send_sem, recv_sem=arrival(kind, v, p),
            device_id=(r2, c2), device_id_type=MESH,
        )

    def send(kind, v, p, buf, r2, c2):
        remote(kind, v, p, buf, r2, c2).start()
        pending.append((kind, v, p, buf))

    def await_part(kind, v, p):
        if (kind, v, p) not in seen:
            seen.add((kind, v, p))
            remote(kind, v, p, inbox[kind], r ^ 1, c).wait_recv()

    def got(kind, v, n):
        await_part(kind, v, part_of(kind, n))
        return inbox[kind][v, n]

    def drain():
        for sent in pending:
            remote(*sent, r ^ 1, c).wait_send()
        pending.clear()
        seen.clear()

    def hello(r2, c2):
        pl.semaphore_signal(barrier, inc=1, device_id=(r2, c2), device_id_type=MESH)

    flag_copies = (
        pltpu.make_async_copy(pattern_in, pattern, flag_sem.at[0]),
        pltpu.make_async_copy(dropped_in, dropped, flag_sem.at[1]),
    )

    def start_flags():
        for copy in flag_copies:
            copy.start()

    FIRST, SECOND, MATRIX, INVERSE = range(4)
    inverse_copy = pltpu.make_async_copy(inverse_in, inverse, load_sem.at[INVERSE])

    def start_loads(group, places):
        source, dest = (matrix, a) if group == MATRIX else (factors, out)
        for i, s, j in places:
            src = (pl.ds(i * bs, bs), pl.ds(pl.multiple_of(j * bs, bs), bs))
            pltpu.make_async_copy(source.at[src], dest.at[i * SLOTS + s], load_sem.at[group]).start()

    def wait_loads(group, places):
        dest = (a if group == MATRIX else out).at[pl.ds(0, len(places))]
        pltpu.make_async_copy(dest, dest, load_sem.at[group]).wait()

    odd = lax.rem(c, 2) == 1

    def lower_step(k, b, v, diag, j, mask=None):
        product = dot(lb[v, b], diag)
        residual = a[k].astype(F32) - product
        if mask is not None:
            residual = residual * mask
        correction = dot(residual.astype(BF16), inverse[j])
        if mask is not None:
            correction = correction * mask
        new = out[k] + correction
        out[k] = new
        if v + 1 < SWEEPS:
            lb[v + 1, b] = new.astype(BF16)

    def upper_steps(k, b, mask=None):
        target, value = a[k].astype(F32), out[k]
        for v in range(SWEEPS):
            residual = target - value
            if mask is not None:
                residual = residual * mask
            value = value + residual
            if v + 1 < SWEEPS:
                ub[v + 1, b] = value.astype(BF16)
        out[k] = value

    def keep(places):
        for i, s, j in places:
            k = i * SLOTS + s
            out[k] = out[k] * (1 - dropped[i, j]).astype(F32)

    def diagonal_owner(h, near_in, far_in, near_out, far_out, detour=False):
        if near_in:
            hello(r - 1, c)
            if not h:
                hello(r, c - 1)
                pl.when(~odd & (c >= 2) & (c < last))(lambda: hello(r + 1, c + 1))
                if far_in:
                    hello(r - 1, c - 2)
        if far_in:
            hello(r - far_r, c)
            hello(r, c - far_c)

        base = h * rows
        left = [(i, LEFT, base + i - 1) for i in range(rows) if base + i >= 1]
        right = [(i, RIGHT, base + i + 1) for i in range(rows) if base + i + 1 < cols]
        diag = [(i, DIAG, base + i) for i in range(rows)]
        outer = [(i, OUTER, i if h else rows + i) for i in range(rows)]
        at_right = lambda i: 0 if i == rows - 1 else 1 + rows + i
        at_left = lambda i: rows + i if i else 0

        start_loads(FIRST, diag)
        start_loads(SECOND, right + outer + left)
        start_loads(MATRIX, right + outer + diag + left)
        inverse_copy.start()
        start_flags()

        wait_loads(FIRST, diag)
        for i in range(rows):
            sd[0, i] = out[i * SLOTS + DIAG].astype(BF16)
        if near_out or far_out:
            pl.semaphore_wait(barrier, near_out + far_out)

        def send_near(v, i):
            if near_out:
                send(D, v, i, sd, r + 1 - detour, c + detour)

        def send_far(v):
            if far_out:
                for i in range(rows):
                    send(D, v, i, sd, r + far_r, c)

        for i in range(rows):
            send_near(0, i)
        send_far(0)

        wait_loads(SECOND, right + outer + left)
        for i, s, j in right:
            ub[0, at_right(i)] = out[i * SLOTS + s].astype(BF16)
        for i, s, j in outer:
            (lb if h else ub)[0, 1 + i] = out[i * SLOTS + s].astype(BF16)
        if not h:
            for p in range(2):
                send(U_NEAR, 0, p, ub, r + 1, c)
        for i, s, j in left:
            lb[0, at_left(i)] = out[i * SLOTS + s].astype(BF16)
        wait_loads(MATRIX, right + outer + diag + left)
        for i, s, j in right if h else right + outer:
            upper_steps(i * SLOTS + s, 1 + i if s == OUTER else at_right(i))
        if not h:
            for p in range(2):
                send(U_NEAR, 1, p, ub, r + 1, c)
        inverse_copy.wait()

        def local_lower(v):
            for i in range(1, rows):
                lower_step(i * SLOTS + LEFT, at_left(i), v, sd[v, i - 1], base + i - 1)

        def lower_from_before(v):
            for i in range(rows):
                from_before = got(D, v, i)
                lower_step(i * SLOTS + OUTER, 1 + i, v, from_before, i)
            lower_step(LEFT, 0, v, from_before, rows - 1)

        def products(v):
            for i in range(1, rows):
                acc[i] = dot(lb[v, at_left(i)], ub[v, at_right(i - 1)])

        def diag_step(v, i):
            k = i * SLOTS + DIAG
            terms = [acc[i]] if i else []
            if near_in:
                for n in (1 + i,) if i else (0, 1):
                    u = got(U_NEAR, v, n)
                    l = lb[v, n] if h else got(L_NEAR, v, n)
                    terms.append(dot(l, u))
            if far_in:
                l = got(L_FAR, v, i)
                u = got(U_FAR, v, i)
                terms.append(dot(l, u))
            old = out[k]
            new = old + (a[k].astype(F32) - sum(terms[1:], terms[0] if terms else jnp.zeros((bs, bs), F32)) - old)
            out[k] = new
            if v + 1 < SWEEPS:
                sd[v + 1, i] = new.astype(BF16)
                send_near(v + 1, i)

        def sweep(v):
            local_lower(v)
            if h:
                lower_from_before(v)
            for i in range(rows) if v + 1 < SWEEPS else (1, 0, *range(2, rows)):
                diag_step(v, i)
            if v + 1 < SWEEPS:
                send_far(v + 1)

        for v in range(SWEEPS):
            pl.when(c >= 0)(lambda: products(v))
            pl.when(c >= 0)(lambda: sweep(v))

        for copy in flag_copies:
            copy.wait()
        keep(left + right + outer)
        drain()

    def lower_owner(blocks, kind, source, target):
        hello(source[0], source[1] + (c == 0).astype(jnp.int32) if kind == L_NEAR else source[1])
        start_flags()
        places = [(i, s, j) for i, s, j, b, n in blocks]
        start_loads(FIRST, places)
        start_loads(MATRIX, places)
        inverse_copy.start()
        if kind == L_FAR:
            flag_copies[0].wait()
        wait_loads(FIRST, places)
        masks = {}
        for i, s, j, b, n in blocks:
            k = i * SLOTS + s
            masks[k] = pattern[i, j].astype(F32) if kind == L_FAR else None
            value = out[k]
            if kind == L_FAR:
                value = value * masks[k]
                out[k] = value
            lb[0, b] = value.astype(BF16)
        detour = (odd & (c + 2 <= last)).astype(jnp.int32) if kind == L_NEAR else 0
        pl.semaphore_wait(barrier, 1 + detour)
        for p in range(len(parts[kind])):
            send(kind, 0, p, lb, *target)
        wait_loads(MATRIX, places)
        inverse_copy.wait()
        for v in range(SWEEPS):
            ds, done = {}, set()
            for i, s, j, b, n in blocks:
                k = i * SLOTS + s
                if n not in ds:
                    ds[n] = got(D, v, n)
                lower_step(k, b, v, ds[n], j, masks[k])
                done.add(b)
                start, size = parts[kind][part_of(kind, b)]
                if v + 1 < SWEEPS and done >= set(range(start, start + size)):
                    send(kind, v + 1, part_of(kind, b), lb, target[0] + detour, target[1] + detour)
        if kind != L_FAR:
            flag_copies[0].wait()
        flag_copies[1].wait()
        keep(places)
        drain()

    def pass_on(kind, v, order, target):
        for p in order:
            await_part(kind, v, p)
            send(kind, v, p, inbox[kind], *target)

    def lead_copies(to, which):
        short = bs // 8
        pieces = ((0, 0, pl.ds(0, short)), (0, 0, pl.ds(short, bs - short)), (0, pl.ds(1, half)))
        return [
            pltpu.make_async_remote_copy(
                src_ref=ub.at[at], dst_ref=run.at[at],
                send_sem=send_sem if n else lead_sem, recv_sem=arrival(U_NEAR, 0, 0),
                device_id=to, device_id_type=MESH,
            )
            for n, at in enumerate(pieces) if n in which
        ]

    def upper_owner(blocks, kind, target, second=None, passes=None):
        if passes is not None:
            when, greeted, body = passes
            pl.when(when)(lambda: hello(*greeted))
        start_flags()
        places = [(i, s, j) for i, s, j, b in blocks]
        start_loads(FIRST, places)
        start_loads(MATRIX, places)
        flag_copies[0].wait()
        wait_loads(FIRST, places)
        masks = {}
        for i, s, j, b in blocks:
            k = i * SLOTS + s
            masks[k] = pattern[i, j].astype(F32) if kind == U_FAR else None
            value = out[k]
            if kind == U_FAR:
                value = value * masks[k]
                out[k] = value
            ub[0, b] = value.astype(BF16)
        peers = 1 + (second is not None or kind == U_FAR)
        if passes is not None:
            peers = peers + when.astype(jnp.int32)
        pl.semaphore_wait(barrier, peers)
        if second is None:
            for p in range(2):
                send(kind, 0, p, ub, *target)
        else:
            for copy in lead_copies(target, (0, 1, 2)):
                copy.start()
            send(kind, 0, 1, ub, *target)
            lead_copies(target, (0,))[0].wait_send()
            for h in (0, 1):
                hello(r + 1 + h - far_r, c)
        wait_loads(MATRIX, places)
        for i, s, j, b in blocks:
            upper_steps(i * SLOTS + s, b, masks[i * SLOTS + s])
        send(kind, 1, 0, ub, *target)
        send(kind, 1, 1, ub, *(second or target))
        flag_copies[1].wait()
        keep(places)
        if passes is not None:
            @pl.when(when)
            def _():
                own = list(pending)
                pending.clear()
                body()
                drain()
                pending.extend(own)
        if second is not None:
            for copy in lead_copies(target, (1, 2)):
                copy.wait_send()
        drain()

    def pass_diagonal():
        for v in range(SWEEPS):
            pass_on(D, v, range(rows), (r + 1, c - 1))

    def near_passer():
        hello(r, c + 2)
        pl.semaphore_wait(barrier, 1)
        pass_on(U_NEAR, 1, (1,), (r + 1, c + 2))
        drain()

    for h in (0, 1):
        pl.when((q == h) & (c == 0))(lambda: diagonal_owner(h, bool(h), False, True, True, bool(h)))
        pl.when((q == h) & (c > 0) & (c < far_c))(lambda: diagonal_owner(h, True, False, True, True))
        pl.when((q == h) & (c >= far_c) & (c < last))(lambda: diagonal_owner(h, True, True, True, False))
        pl.when((q == h) & (c == last))(lambda: diagonal_owner(h, True, True, not h, False))

    near_lower = [(i, OUTER, rows + i, 1 + i, i) for i in range(rows)] + [(0, LEFT, cols - 1, 0, rows - 1)]
    pl.when(q == 2)(lambda: lower_owner(near_lower, L_NEAR, (r - 1, c), (r, c + 1)))

    near_upper = [(rows - 1, RIGHT, 0, 0)] + [(i, OUTER, i, 1 + i) for i in range(rows)]
    pass_lower = (odd & (c >= 3), (r - 1, c - 2), lambda: pass_on(L_NEAR, 1, (*range(1, rows + 1), 0), (r - 1, c - 1)))
    pass_diag = (c == 1, (r, c - 1), pass_diagonal)
    pl.when((q == -1) & (c == 1))(lambda: upper_owner(near_upper, U_NEAR, (r + 1, c), passes=pass_diag))
    pl.when((q == -1) & (c > 1) & (c < far_c))(lambda: upper_owner(near_upper, U_NEAR, (r + 1, c), passes=pass_lower))
    pl.when((q == -1) & (c >= far_c))(
        lambda: upper_owner(near_upper, U_NEAR, (r + 1, c), second=(r, c - 2), passes=pass_lower)
    )
    pl.when((q == 3) & (c + 2 >= far_c) & (c + 2 <= last))(near_passer)
    for h in (0, 1):
        far_lower = [(i, OUTER, h * rows + i, i, i) for i in range(rows)]
        far_upper = [(i, OUTER, h * rows + i, i) for i in range(rows)]
        pl.when(q == far_r + h)(lambda: lower_owner(far_lower, L_FAR, (r - far_r, c), (r, c + far_c)))
        pl.when(q == h - far_r)(
            lambda: upper_owner(far_upper, U_FAR, (r + far_r, c))
        )

    out[rows * SLOTS] = jnp.zeros((bs, bs), F32)


def place_kernel(rows, cols, row_devices, bs, blocks, out, sem):
    r, c = lax.axis_index("row"), lax.axis_index("col")
    q = r - (cols // rows) * c
    far = (row_devices // 2) * rows
    copies = []
    for i in range(rows):
        for j in range(cols):
            d = rows * q + i - j
            k = jnp.where(
                d == 0, i * SLOTS + DIAG,
                jnp.where(
                    d == 1, i * SLOTS + LEFT,
                    jnp.where(
                        d == -1, i * SLOTS + RIGHT,
                        jnp.where(
                            (d == rows) | (d == -rows) | (d == far) | (d == -far),
                            i * SLOTS + OUTER, rows * SLOTS,
                        ),
                    ),
                ),
            )
            dst = out.at[pl.ds(i * bs, bs), pl.ds(j * bs, bs)]
            copies.append(pltpu.make_async_copy(blocks.at[k], dst, sem))
    for copy in copies:
        copy.start()
    pltpu.make_async_copy(out, out, sem).wait()


def solution(mesh):
    row_devices, col_devices = mesh.shape["row"], mesh.shape["col"]

    def on_device(matrix, factors, inverse, pattern, dropped):
        rows, cols = pattern.shape
        bs = inverse.shape[1]
        places = rows * SLOTS
        half = lambda *n: pltpu.VMEM(n + (bs, bs), BF16)
        hbm = pl.BlockSpec(memory_space=pl.ANY)
        vmem = pl.BlockSpec(memory_space=pltpu.VMEM)
        blocks = pl.pallas_call(
            functools.partial(sweep_kernel, rows, cols, row_devices, col_devices, bs),
            out_shape=pltpu.VMEM((places + 1, bs, bs), F32),
            in_specs=[hbm] * 5,
            out_specs=vmem,
            scratch_shapes=[
                pltpu.SMEM((rows, cols), jnp.int32), pltpu.SMEM((rows, cols), jnp.int32),
                half(places), half(cols), half(SWEEPS, 2 * rows), half(SWEEPS, 2 * rows),
                half(SWEEPS, rows), half(SWEEPS, rows),
                half(SWEEPS, rows + 1), half(SWEEPS, rows + 1), half(SWEEPS, rows), half(SWEEPS, rows),
                pltpu.VMEM((rows, bs, bs), F32),
                pltpu.SemaphoreType.DMA((2,)),
                pltpu.SemaphoreType.DMA((4,)),
                pltpu.SemaphoreType.DMA,
                pltpu.SemaphoreType.DMA,
                pltpu.SemaphoreType.DMA((SWEEPS * (rows + 7),)),
            ],
            compiler_params=pltpu.CompilerParams(collective_id=0, has_side_effects=True),
            name="sweeps",
        )(pattern, dropped, matrix, factors, inverse)
        return pl.pallas_call(
            functools.partial(place_kernel, rows, cols, row_devices, bs),
            out_shape=jax.ShapeDtypeStruct(factors.shape, F32),
            in_specs=[vmem],
            out_specs=hbm,
            scratch_shapes=[pltpu.SemaphoreType.DMA],
            name="place",
        )(pltpu.with_memory_space_constraint(blocks, pltpu.VMEM))

    placed = (P("row", "col"), P("row", "col"), P("col", None, None), P("row", "col"), P("row", "col"))
    return jax.shard_map(
        on_device, mesh=mesh, in_specs=placed, out_specs=P("row", "col"), check_vma=False
    )
```

```python
import functools

import jax
import jax.numpy as jnp
from jax import lax
from jax.experimental import pallas as pl
from jax.experimental.pallas import tpu as pltpu
from jax.sharding import PartitionSpec as P

SWEEPS = 2
MESH = pl.DeviceIdType.MESH
F32 = jnp.float32
BF16 = jnp.bfloat16

SLOTS = 4
DIAG, LEFT, RIGHT, OUTER = range(SLOTS)
D, L_NEAR, U_NEAR, L_FAR, U_FAR = range(5)
DETOURED = ((), ())

def dot(x, y):
    return jnp.dot(x, y, preferred_element_type=F32)


def sweep_kernel(
    rows, cols, row_devices, col_devices, bs,
    pattern_in, dropped_in, matrix, factors, inverse_in, out,
    pattern, dropped, a, inverse, lb, ub, sd, rd, rln, run, rlf, ruf, acc,
    flag_sem, load_sem, lead_sem, send_sem, recv_sem,
):
    r, c = lax.axis_index("row"), lax.axis_index("col")
    far_r, far_c = row_devices // 2, col_devices // 2
    last = col_devices - 1
    q = r - (cols // rows) * c
    barrier = pltpu.get_barrier_semaphore()
    inbox = {D: rd, L_NEAR: rln, U_NEAR: run, L_FAR: rlf, U_FAR: ruf}
    half = rows // 2

    near = [(0, 1 + half), (1 + half, rows - half)]
    far = [(0, half), (half, rows - half)]
    parts = {
        D: [(n, 1) for n in range(rows)], L_NEAR: [(n, 1) for n in range(rows + 1)],
        U_NEAR: near, L_FAR: far, U_FAR: far,
    }
    first_sem = {D: 0, L_NEAR: 0}
    for kind, before, size in ((U_NEAR, L_NEAR, rows + 1), (L_FAR, U_NEAR, 2), (U_FAR, L_FAR, 2)):
        first_sem[kind] = first_sem[before] + SWEEPS * size

    def arrival(kind, v, p):
        size = rows + 1 if kind in (D, L_NEAR) else 2
        return recv_sem.at[first_sem[kind] + v * size + p]

    def part_of(kind, n):
        return max(p for p, (start, size) in enumerate(parts[kind]) if start <= n)

    pending, seen = [], set()

    def remote(kind, v, p, buf, r2, c2):
        at = (v, pl.ds(*parts[kind][p]))
        return pltpu.make_async_remote_copy(
            src_ref=buf.at[at], dst_ref=inbox[kind].at[at],
            send_sem=send_sem, recv_sem=arrival(kind, v, p),
            device_id=(r2, c2), device_id_type=MESH,
        )

    def send(kind, v, p, buf, r2, c2):
        remote(kind, v, p, buf, r2, c2).start()
        pending.append((kind, v, p, buf))

    def await_part(kind, v, p):
        if (kind, v, p) not in seen:
            seen.add((kind, v, p))
            remote(kind, v, p, inbox[kind], r ^ 1, c).wait_recv()

    def got(kind, v, n):
        await_part(kind, v, part_of(kind, n))
        return inbox[kind][v, n]

    def drain():
        for sent in pending:
            remote(*sent, r ^ 1, c).wait_send()
        pending.clear()
        seen.clear()

    def hello(r2, c2):
        pl.semaphore_signal(barrier, inc=1, device_id=(r2, c2), device_id_type=MESH)

    flag_copies = (
        pltpu.make_async_copy(pattern_in, pattern, flag_sem.at[0]),
        pltpu.make_async_copy(dropped_in, dropped, flag_sem.at[1]),
    )

    def start_flags():
        for copy in flag_copies:
            copy.start()

    FIRST, SECOND, MATRIX, INVERSE = range(4)
    inverse_copy = pltpu.make_async_copy(inverse_in, inverse, load_sem.at[INVERSE])

    def start_loads(group, places):
        source, dest = (matrix, a) if group == MATRIX else (factors, out)
        for i, s, j in places:
            src = (pl.ds(i * bs, bs), pl.ds(pl.multiple_of(j * bs, bs), bs))
            pltpu.make_async_copy(source.at[src], dest.at[i * SLOTS + s], load_sem.at[group]).start()

    def wait_loads(group, places):
        dest = (a if group == MATRIX else out).at[pl.ds(0, len(places))]
        pltpu.make_async_copy(dest, dest, load_sem.at[group]).wait()

    odd = lax.rem(c, 2) == 1
    aside = odd.astype(jnp.int32)

    def lower_step(k, b, v, diag, j, mask=None):
        product = dot(lb[v, b], diag)
        residual = a[k].astype(F32) - product
        if mask is not None:
            residual = residual * mask
        correction = dot(residual.astype(BF16), inverse[j])
        if mask is not None:
            correction = correction * mask
        new = out[k] + correction
        out[k] = new
        if v + 1 < SWEEPS:
            lb[v + 1, b] = new.astype(BF16)

    def upper_steps(k, b, mask=None):
        target, value = a[k].astype(F32), out[k]
        for v in range(SWEEPS):
            residual = target - value
            if mask is not None:
                residual = residual * mask
            value = value + residual
            if v + 1 < SWEEPS:
                ub[v + 1, b] = value.astype(BF16)
        out[k] = value

    def keep(places):
        for i, s, j in places:
            k = i * SLOTS + s
            out[k] = out[k] * (1 - dropped[i, j]).astype(F32)

    def diagonal_owner(h, near_in, far_in, near_out, far_out, detour=False):
        if near_in:
            hello(r - 1, c)
            if not h:
                hello(r, c - 1)
                pl.when(~odd & (c >= 2) & (c < last))(lambda: hello(r + 1, c + 1))
                if far_in:
                    hello(r - 1, c - 2)
        if far_in:
            hello(r - far_r, c)
            hello(r, c - far_c)

        base = h * rows
        left = [(i, LEFT, base + i - 1) for i in range(rows) if base + i >= 1]
        right = [(i, RIGHT, base + i + 1) for i in range(rows) if base + i + 1 < cols]
        diag = [(i, DIAG, base + i) for i in range(rows)]
        outer = [(i, OUTER, i if h else rows + i) for i in range(rows)]
        at_right = lambda i: 0 if i == rows - 1 else 1 + rows + i
        at_left = lambda i: rows + i if i else 0

        start_loads(FIRST, diag)
        start_loads(SECOND, right + outer + left)
        start_loads(MATRIX, right + outer + diag + left)
        inverse_copy.start()
        start_flags()

        wait_loads(FIRST, diag)
        for i in range(rows):
            sd[0, i] = out[i * SLOTS + DIAG].astype(BF16)
        if near_out or far_out:
            pl.semaphore_wait(barrier, near_out + far_out + bool(detour) + (aside if h and far_out and not detour else 0))

        def send_near(v, i):
            if near_out:
                if detour and (v or i >= 2):
                    send(D, v, i, sd, r, c + 1)
                elif h and far_out and near_in and not detour and i in DETOURED[v]:
                    send(D, v, i, sd, r + 1 - aside, c - aside)
                else:
                    send(D, v, i, sd, r + 1, c)

        def send_far(v):
            if far_out:
                for i in range(rows):
                    send(D, v, i, sd, r + far_r, c)

        for i in range(rows):
            send_near(0, i)
        send_far(0)

        wait_loads(SECOND, right + outer + left)
        for i, s, j in right:
            ub[0, at_right(i)] = out[i * SLOTS + s].astype(BF16)
        for i, s, j in outer:
            (lb if h else ub)[0, 1 + i] = out[i * SLOTS + s].astype(BF16)
        if not h:
            for p in range(2):
                send(U_NEAR, 0, p, ub, r + 1, c)
        for i, s, j in left:
            lb[0, at_left(i)] = out[i * SLOTS + s].astype(BF16)
        wait_loads(MATRIX, right + outer + diag + left)
        for i, s, j in right if h else right + outer:
            upper_steps(i * SLOTS + s, 1 + i if s == OUTER else at_right(i))
        if not h:
            for p in range(2):
                send(U_NEAR, 1, p, ub, r + 1, c)
        inverse_copy.wait()

        def local_lower(v):
            for i in range(1, rows):
                lower_step(i * SLOTS + LEFT, at_left(i), v, sd[v, i - 1], base + i - 1)

        def lower_from_before(v):
            for i in range(rows):
                from_before = got(D, v, i)
                lower_step(i * SLOTS + OUTER, 1 + i, v, from_before, i)
            lower_step(LEFT, 0, v, from_before, rows - 1)

        def products(v):
            for i in range(1, rows):
                acc[i] = dot(lb[v, at_left(i)], ub[v, at_right(i - 1)])

        def diag_step(v, i):
            k = i * SLOTS + DIAG
            terms = [acc[i]] if i else []
            if near_in:
                for n in (1 + i,) if i else (0, 1):
                    u = got(U_NEAR, v, n)
                    l = lb[v, n] if h else got(L_NEAR, v, n)
                    terms.append(dot(l, u))
            if far_in:
                l = got(L_FAR, v, i)
                u = got(U_FAR, v, i)
                terms.append(dot(l, u))
            old = out[k]
            new = old + (a[k].astype(F32) - sum(terms[1:], terms[0] if terms else jnp.zeros((bs, bs), F32)) - old)
            out[k] = new
            if v + 1 < SWEEPS:
                sd[v + 1, i] = new.astype(BF16)
                send_near(v + 1, i)

        def sweep(v):
            local_lower(v)
            if h:
                lower_from_before(v)
            for i in range(rows) if v + 1 < SWEEPS else (1, 0, *range(2, rows)):
                diag_step(v, i)
            if v + 1 < SWEEPS:
                send_far(v + 1)

        for v in range(SWEEPS):
            pl.when(c >= 0)(lambda: products(v))
            pl.when(c >= 0)(lambda: sweep(v))

        for copy in flag_copies:
            copy.wait()
        keep(left + right + outer)
        drain()

    def lower_owner(blocks, kind, source, target):
        hello(*source)
        if kind == L_NEAR:
            pl.when(c == 0)(lambda: hello(r - 1, c + 1))
            pl.when(odd & (c < far_c))(lambda: hello(r - 1, c - 1))
        start_flags()
        places = [(i, s, j) for i, s, j, b, n in blocks]
        start_loads(FIRST, places)
        start_loads(MATRIX, places)
        inverse_copy.start()
        if kind == L_FAR:
            flag_copies[0].wait()
        wait_loads(FIRST, places)
        masks = {}
        for i, s, j, b, n in blocks:
            k = i * SLOTS + s
            masks[k] = pattern[i, j].astype(F32) if kind == L_FAR else None
            value = out[k]
            if kind == L_FAR:
                value = value * masks[k]
                out[k] = value
            lb[0, b] = value.astype(BF16)
        detour = (odd & (c + 2 <= last)).astype(jnp.int32) if kind == L_NEAR else 0
        pl.semaphore_wait(barrier, 1 + detour)
        for p in range(len(parts[kind])):
            send(kind, 0, p, lb, *target)
        wait_loads(MATRIX, places)
        inverse_copy.wait()
        for v in range(SWEEPS):
            ds, done = {}, set()
            for i, s, j, b, n in blocks:
                k = i * SLOTS + s
                if n not in ds:
                    ds[n] = got(D, v, n)
                lower_step(k, b, v, ds[n], j, masks[k])
                done.add(b)
                start, size = parts[kind][part_of(kind, b)]
                if v + 1 < SWEEPS and done >= set(range(start, start + size)):
                    send(kind, v + 1, part_of(kind, b), lb, target[0] + detour, target[1] + detour)
        if kind != L_FAR:
            flag_copies[0].wait()
        flag_copies[1].wait()
        keep(places)
        drain()

    def pass_on(kind, v, order, target):
        for p in order:
            await_part(kind, v, p)
            send(kind, v, p, inbox[kind], *target)

    def lead_copies(to, which):
        short = bs // 8
        pieces = ((0, 0, pl.ds(0, short)), (0, 0, pl.ds(short, bs - short)), (0, pl.ds(1, half)))
        return [
            pltpu.make_async_remote_copy(
                src_ref=ub.at[at], dst_ref=run.at[at],
                send_sem=send_sem if n else lead_sem, recv_sem=arrival(U_NEAR, 0, 0),
                device_id=to, device_id_type=MESH,
            )
            for n, at in enumerate(pieces) if n in which
        ]

    def upper_owner(blocks, kind, target, second=None, passes=None):
        if passes is not None:
            when, greeted, body = passes
            pl.when(when)(lambda: hello(*greeted))
        start_flags()
        places = [(i, s, j) for i, s, j, b in blocks]
        start_loads(FIRST, places)
        start_loads(MATRIX, places)
        flag_copies[0].wait()
        wait_loads(FIRST, places)
        masks = {}
        for i, s, j, b in blocks:
            k = i * SLOTS + s
            masks[k] = pattern[i, j].astype(F32) if kind == U_FAR else None
            value = out[k]
            if kind == U_FAR:
                value = value * masks[k]
                out[k] = value
            ub[0, b] = value.astype(BF16)
        peers = 1 + (second is not None or kind == U_FAR)
        if passes is not None:
            peers = peers + when.astype(jnp.int32)
        pl.semaphore_wait(barrier, peers)
        if second is None:
            for p in range(2):
                send(kind, 0, p, ub, *target)
        else:
            for copy in lead_copies(target, (0, 1, 2)):
                copy.start()
            send(kind, 0, 1, ub, *target)
            lead_copies(target, (0,))[0].wait_send()
            for h in (0, 1):
                hello(r + 1 + h - far_r, c)
        wait_loads(MATRIX, places)
        for i, s, j, b in blocks:
            upper_steps(i * SLOTS + s, b, masks[i * SLOTS + s])
        send(kind, 1, 0, ub, *(second or target))
        send(kind, 1, 1, ub, *target)
        flag_copies[1].wait()
        keep(places)
        if passes is not None:
            @pl.when(when)
            def _():
                own = list(pending)
                pending.clear()
                body()
                drain()
                pending.extend(own)
        if second is not None:
            for copy in lead_copies(target, (1, 2)):
                copy.wait_send()
        drain()

    def pass_diagonal():
        pass_on(D, 0, range(2, rows), (r + 1, c - 1))
        pass_on(D, 1, range(rows), (r + 1, c - 1))

    def near_passer():
        upper = (c + 2 >= far_c) & (c + 2 <= last)
        diag = ~odd & (c + 1 < far_c)
        pl.when(upper)(lambda: hello(r, c + 2))
        pl.when(diag)(lambda: hello(r, c + 1))
        pl.semaphore_wait(barrier, upper.astype(jnp.int32) + diag.astype(jnp.int32))
        sent = {}

        def step(when, name, *what):
            pl.when(when)(lambda: pass_on(*what))
            sent.setdefault(name, (when, []))[1].extend(pending)
            pending.clear()

        if DETOURED[0]:
            step(diag, D, D, 0, DETOURED[0], (r + 1, c + 1))
        step(upper, U_NEAR, U_NEAR, 1, (0,), (r + 1, c + 2))
        if DETOURED[1]:
            step(diag, D, D, 1, DETOURED[1], (r + 1, c + 1))
        for when, own in sent.values():
            pending.extend(own)
            pl.when(when)(drain)
            pending.clear()

    for h in (0, 1):
        pl.when((q == h) & (c == 0))(lambda: diagonal_owner(h, bool(h), False, True, True, bool(h)))
        pl.when((q == h) & (c > 0) & (c < far_c))(lambda: diagonal_owner(h, True, False, True, True))
        pl.when((q == h) & (c >= far_c) & (c < last))(lambda: diagonal_owner(h, True, True, True, False))
        pl.when((q == h) & (c == last))(lambda: diagonal_owner(h, True, True, not h, False))

    near_lower = [(i, OUTER, rows + i, 1 + i, i) for i in range(rows)] + [(0, LEFT, cols - 1, 0, rows - 1)]
    pl.when(q == 2)(lambda: lower_owner(near_lower, L_NEAR, (r - 1, c), (r, c + 1)))

    near_upper = [(rows - 1, RIGHT, 0, 0)] + [(i, OUTER, i, 1 + i) for i in range(rows)]
    pass_lower = (odd & (c >= 3), (r - 1, c - 2), lambda: pass_on(L_NEAR, 1, (*range(1, rows + 1), 0), (r - 1, c - 1)))
    pass_diag = (c == 1, (r, c - 1), pass_diagonal)
    pl.when((q == -1) & (c == 1))(lambda: upper_owner(near_upper, U_NEAR, (r + 1, c), passes=pass_diag))
    pl.when((q == -1) & (c > 1) & (c < far_c))(lambda: upper_owner(near_upper, U_NEAR, (r + 1, c), passes=pass_lower))
    pl.when((q == -1) & (c >= far_c))(
        lambda: upper_owner(near_upper, U_NEAR, (r + 1, c), second=(r, c - 2), passes=pass_lower)
    )
    pl.when((q == 3) & (c + 2 <= last))(near_passer)
    for h in (0, 1):
        far_lower = [(i, OUTER, h * rows + i, i, i) for i in range(rows)]
        far_upper = [(i, OUTER, h * rows + i, i) for i in range(rows)]
        pl.when(q == far_r + h)(lambda: lower_owner(far_lower, L_FAR, (r - far_r, c), (r, c + far_c)))
        pl.when(q == h - far_r)(
            lambda: upper_owner(far_upper, U_FAR, (r + far_r, c))
        )

    out[rows * SLOTS] = jnp.zeros((bs, bs), F32)


def place_kernel(rows, cols, row_devices, bs, blocks, out, sem):
    r, c = lax.axis_index("row"), lax.axis_index("col")
    q = r - (cols // rows) * c
    far = (row_devices // 2) * rows
    copies = []
    for i in range(rows):
        for j in range(cols):
            d = rows * q + i - j
            k = jnp.where(
                d == 0, i * SLOTS + DIAG,
                jnp.where(
                    d == 1, i * SLOTS + LEFT,
                    jnp.where(
                        d == -1, i * SLOTS + RIGHT,
                        jnp.where(
                            (d == rows) | (d == -rows) | (d == far) | (d == -far),
                            i * SLOTS + OUTER, rows * SLOTS,
                        ),
                    ),
                ),
            )
            dst = out.at[pl.ds(i * bs, bs), pl.ds(j * bs, bs)]
            copies.append(pltpu.make_async_copy(blocks.at[k], dst, sem))
    for copy in copies:
        copy.start()
    pltpu.make_async_copy(out, out, sem).wait()


def solution(mesh):
    row_devices, col_devices = mesh.shape["row"], mesh.shape["col"]

    def on_device(matrix, factors, inverse, pattern, dropped):
        rows, cols = pattern.shape
        bs = inverse.shape[1]
        places = rows * SLOTS
        half = lambda *n: pltpu.VMEM(n + (bs, bs), BF16)
        hbm = pl.BlockSpec(memory_space=pl.ANY)
        vmem = pl.BlockSpec(memory_space=pltpu.VMEM)
        blocks = pl.pallas_call(
            functools.partial(sweep_kernel, rows, cols, row_devices, col_devices, bs),
            out_shape=pltpu.VMEM((places + 1, bs, bs), F32),
            in_specs=[hbm] * 5,
            out_specs=vmem,
            scratch_shapes=[
                pltpu.SMEM((rows, cols), jnp.int32), pltpu.SMEM((rows, cols), jnp.int32),
                half(places), half(cols), half(SWEEPS, 2 * rows), half(SWEEPS, 2 * rows),
                half(SWEEPS, rows), half(SWEEPS, rows),
                half(SWEEPS, rows + 1), half(SWEEPS, rows + 1), half(SWEEPS, rows), half(SWEEPS, rows),
                pltpu.VMEM((rows, bs, bs), F32),
                pltpu.SemaphoreType.DMA((2,)),
                pltpu.SemaphoreType.DMA((4,)),
                pltpu.SemaphoreType.DMA,
                pltpu.SemaphoreType.DMA,
                pltpu.SemaphoreType.DMA((SWEEPS * (rows + 7),)),
            ],
            compiler_params=pltpu.CompilerParams(collective_id=0, has_side_effects=True),
            name="sweeps",
        )(pattern, dropped, matrix, factors, inverse)
        return pl.pallas_call(
            functools.partial(place_kernel, rows, cols, row_devices, bs),
            out_shape=jax.ShapeDtypeStruct(factors.shape, F32),
            in_specs=[vmem],
            out_specs=hbm,
            scratch_shapes=[pltpu.SemaphoreType.DMA],
            name="place",
        )(pltpu.with_memory_space_constraint(blocks, pltpu.VMEM))

    placed = (P("row", "col"), P("row", "col"), P("col", None, None), P("row", "col"), P("row", "col"))
    return jax.shard_map(
        on_device, mesh=mesh, in_specs=placed, out_specs=P("row", "col"), check_vma=False
    )
```

```python
import functools

import jax
import jax.numpy as jnp
from jax import lax
from jax.experimental import pallas as pl
from jax.experimental.pallas import tpu as pltpu
from jax.sharding import PartitionSpec as P

SWEEPS = 2
MESH = pl.DeviceIdType.MESH
F32 = jnp.float32
BF16 = jnp.bfloat16

SLOTS = 4
DIAG, LEFT, RIGHT, OUTER = range(SLOTS)
D, L_NEAR, U_NEAR, L_FAR, U_FAR = range(5)
DETOURED = ((), ())

def dot(x, y):
    return jnp.dot(x, y, preferred_element_type=F32)


def sweep_kernel(
    rows, cols, row_devices, col_devices, bs,
    pattern_in, dropped_in, matrix, factors, inverse_in, out,
    pattern, dropped, a, inverse, lb, ub, sd, rd, rln, run, rlf, ruf, acc,
    flag_sem, load_sem, lead_sem, send_sem, recv_sem,
):
    r, c = lax.axis_index("row"), lax.axis_index("col")
    far_r, far_c = row_devices // 2, col_devices // 2
    last = col_devices - 1
    q = r - (cols // rows) * c
    barrier = pltpu.get_barrier_semaphore()
    inbox = {D: rd, L_NEAR: rln, U_NEAR: run, L_FAR: rlf, U_FAR: ruf}
    half = rows // 2

    near = [(0, 1 + half), (1 + half, rows - half)]
    far = [(0, half), (half, rows - half)]
    parts = {
        D: [(n, 1) for n in range(rows)], L_NEAR: [(n, 1) for n in range(rows + 1)],
        U_NEAR: near, L_FAR: far, U_FAR: far,
    }
    first_sem = {D: 0, L_NEAR: 0}
    for kind, before, size in ((U_NEAR, L_NEAR, rows + 1), (L_FAR, U_NEAR, 2), (U_FAR, L_FAR, 2)):
        first_sem[kind] = first_sem[before] + SWEEPS * size

    def arrival(kind, v, p):
        size = rows + 1 if kind in (D, L_NEAR) else 2
        return recv_sem.at[first_sem[kind] + v * size + p]

    def part_of(kind, n):
        return max(p for p, (start, size) in enumerate(parts[kind]) if start <= n)

    pending, seen = [], set()

    def remote(kind, v, p, buf, r2, c2, block=None):
        at = (v, pl.ds(*(parts[kind][p] if block is None else (block, 1))))
        return pltpu.make_async_remote_copy(
            src_ref=buf.at[at], dst_ref=inbox[kind].at[at],
            send_sem=send_sem, recv_sem=arrival(kind, v, p),
            device_id=(r2, c2), device_id_type=MESH,
        )

    def send(kind, v, p, buf, r2, c2, block=None):
        remote(kind, v, p, buf, r2, c2, block).start()
        pending.append((kind, v, p, buf, block))

    def await_part(kind, v, p):
        if (kind, v, p) not in seen:
            seen.add((kind, v, p))
            remote(kind, v, p, inbox[kind], r ^ 1, c).wait_recv()

    def got(kind, v, n):
        await_part(kind, v, part_of(kind, n))
        return inbox[kind][v, n]

    def drain():
        for kind, v, p, buf, block in pending:
            remote(kind, v, p, buf, r ^ 1, c, block).wait_send()
        pending.clear()
        seen.clear()

    def hello(r2, c2):
        pl.semaphore_signal(barrier, inc=1, device_id=(r2, c2), device_id_type=MESH)

    flag_copies = (
        pltpu.make_async_copy(pattern_in, pattern, flag_sem.at[0]),
        pltpu.make_async_copy(dropped_in, dropped, flag_sem.at[1]),
    )

    def start_flags():
        for copy in flag_copies:
            copy.start()

    FIRST, SECOND, MATRIX, INVERSE = range(4)
    inverse_copy = pltpu.make_async_copy(inverse_in, inverse, load_sem.at[INVERSE])

    def start_loads(group, places):
        source, dest = (matrix, a) if group == MATRIX else (factors, out)
        for i, s, j in places:
            src = (pl.ds(i * bs, bs), pl.ds(pl.multiple_of(j * bs, bs), bs))
            pltpu.make_async_copy(source.at[src], dest.at[i * SLOTS + s], load_sem.at[group]).start()

    def wait_loads(group, places):
        dest = (a if group == MATRIX else out).at[pl.ds(0, len(places))]
        pltpu.make_async_copy(dest, dest, load_sem.at[group]).wait()

    odd = lax.rem(c, 2) == 1
    aside = odd.astype(jnp.int32)

    def lower_step(k, b, v, diag, j, mask=None):
        product = dot(lb[v, b], diag)
        residual = a[k].astype(F32) - product
        if mask is not None:
            residual = residual * mask
        correction = dot(residual.astype(BF16), inverse[j])
        if mask is not None:
            correction = correction * mask
        new = out[k] + correction
        out[k] = new
        if v + 1 < SWEEPS:
            lb[v + 1, b] = new.astype(BF16)

    def upper_steps(k, b, mask=None):
        target, value = a[k].astype(F32), out[k]
        for v in range(SWEEPS):
            residual = target - value
            if mask is not None:
                residual = residual * mask
            value = value + residual
            if v + 1 < SWEEPS:
                ub[v + 1, b] = value.astype(BF16)
        out[k] = value

    def keep(places):
        for i, s, j in places:
            k = i * SLOTS + s
            out[k] = out[k] * (1 - dropped[i, j]).astype(F32)

    def diagonal_owner(h, near_in, far_in, near_out, far_out, detour=False):
        if near_in:
            hello(r - 1, c)
            if not h:
                hello(r, c - 1)
                pl.when(~odd & (c >= 2) & (c < last))(lambda: hello(r + 1, c + 1))
                if far_in:
                    hello(r - 1, c - 2)
        if far_in:
            hello(r - far_r, c)
            hello(r, c - far_c)

        base = h * rows
        left = [(i, LEFT, base + i - 1) for i in range(rows) if base + i >= 1]
        right = [(i, RIGHT, base + i + 1) for i in range(rows) if base + i + 1 < cols]
        diag = [(i, DIAG, base + i) for i in range(rows)]
        outer = [(i, OUTER, i if h else rows + i) for i in range(rows)]
        at_right = lambda i: 0 if i == rows - 1 else 1 + rows + i
        at_left = lambda i: rows + i if i else 0

        start_loads(FIRST, diag)
        start_loads(SECOND, right + outer + left)
        start_loads(MATRIX, right + outer + diag + left)
        inverse_copy.start()
        start_flags()

        wait_loads(FIRST, diag)
        for i in range(rows):
            sd[0, i] = out[i * SLOTS + DIAG].astype(BF16)
        if near_out or far_out:
            pl.semaphore_wait(barrier, near_out + far_out + bool(detour) + (aside if h and far_out and not detour else 0))

        def send_near(v, i):
            if near_out:
                if detour and (v or i >= 2):
                    send(D, v, i, sd, r, c + 1)
                elif h and far_out and near_in and not detour and i in DETOURED[v]:
                    send(D, v, i, sd, r + 1 - aside, c - aside)
                else:
                    send(D, v, i, sd, r + 1, c)

        def send_far(v):
            if far_out:
                for i in range(rows):
                    send(D, v, i, sd, r + far_r, c)

        for i in range(rows):
            send_near(0, i)
        send_far(0)

        wait_loads(SECOND, right + outer + left)
        for i, s, j in right:
            ub[0, at_right(i)] = out[i * SLOTS + s].astype(BF16)
        for i, s, j in outer:
            (lb if h else ub)[0, 1 + i] = out[i * SLOTS + s].astype(BF16)
        if not h:
            for p in range(2):
                send(U_NEAR, 0, p, ub, r + 1, c)
        for i, s, j in left:
            lb[0, at_left(i)] = out[i * SLOTS + s].astype(BF16)
        wait_loads(MATRIX, right + outer + diag + left)
        for i, s, j in right if h else right + outer:
            upper_steps(i * SLOTS + s, 1 + i if s == OUTER else at_right(i))
        if not h:
            for p in range(2):
                send(U_NEAR, 1, p, ub, r + 1, c)
        inverse_copy.wait()

        def local_lower(v):
            for i in range(1, rows):
                lower_step(i * SLOTS + LEFT, at_left(i), v, sd[v, i - 1], base + i - 1)

        def lower_from_before(v):
            for i in range(rows):
                from_before = got(D, v, i)
                lower_step(i * SLOTS + OUTER, 1 + i, v, from_before, i)
            lower_step(LEFT, 0, v, from_before, rows - 1)

        def products(v):
            for i in range(1, rows):
                acc[i] = dot(lb[v, at_left(i)], ub[v, at_right(i - 1)])

        def diag_step(v, i):
            k = i * SLOTS + DIAG
            terms = [acc[i]] if i else []
            if near_in:
                for n in (1 + i,) if i else (0, 1):
                    u = got(U_NEAR, v, n)
                    l = lb[v, n] if h else got(L_NEAR, v, n)
                    terms.append(dot(l, u))
            if far_in:
                l = got(L_FAR, v, i)
                u = got(U_FAR, v, i)
                terms.append(dot(l, u))
            old = out[k]
            new = old + (a[k].astype(F32) - sum(terms[1:], terms[0] if terms else jnp.zeros((bs, bs), F32)) - old)
            out[k] = new
            if v + 1 < SWEEPS:
                sd[v + 1, i] = new.astype(BF16)
                send_near(v + 1, i)

        def sweep(v):
            local_lower(v)
            if h:
                lower_from_before(v)
            for i in range(rows) if v + 1 < SWEEPS else (1, 0, *range(2, rows)):
                diag_step(v, i)
            if v + 1 < SWEEPS:
                send_far(v + 1)

        for v in range(SWEEPS):
            pl.when(c >= 0)(lambda: products(v))
            pl.when(c >= 0)(lambda: sweep(v))

        for copy in flag_copies:
            copy.wait()
        keep(left + right + outer)
        drain()

    def lower_owner(blocks, kind, source, target):
        hello(*source)
        if kind == L_NEAR:
            pl.when(c == 0)(lambda: hello(r - 1, c + 1))
            pl.when(odd & (c < far_c))(lambda: hello(r - 1, c - 1))
        start_flags()
        places = [(i, s, j) for i, s, j, b, n in blocks]
        start_loads(FIRST, places)
        start_loads(MATRIX, places)
        inverse_copy.start()
        if kind == L_FAR:
            flag_copies[0].wait()
        wait_loads(FIRST, places)
        masks = {}
        for i, s, j, b, n in blocks:
            k = i * SLOTS + s
            masks[k] = pattern[i, j].astype(F32) if kind == L_FAR else None
            value = out[k]
            if kind == L_FAR:
                value = value * masks[k]
                out[k] = value
            lb[0, b] = value.astype(BF16)
        detour = (odd & (c + 2 <= last)).astype(jnp.int32) if kind == L_NEAR else 0
        pl.semaphore_wait(barrier, 1 + detour)
        for p in range(len(parts[kind])):
            send(kind, 0, p, lb, *target)
        wait_loads(MATRIX, places)
        inverse_copy.wait()
        for v in range(SWEEPS):
            ds = {}
            for i, s, j, b, n in blocks:
                k = i * SLOTS + s
                if n not in ds:
                    ds[n] = got(D, v, n)
                lower_step(k, b, v, ds[n], j, masks[k])
                if v + 1 < SWEEPS:
                    send(kind, v + 1, part_of(kind, b), lb, target[0] + detour, target[1] + detour, b)
        if kind != L_FAR:
            flag_copies[0].wait()
        flag_copies[1].wait()
        keep(places)
        drain()

    def pass_on(kind, v, order, target):
        for p in order:
            await_part(kind, v, p)
            send(kind, v, p, inbox[kind], *target)

    def lead_copies(to, which):
        short = bs // 8
        pieces = ((0, 0, pl.ds(0, short)), (0, 0, pl.ds(short, bs - short)), (0, pl.ds(1, half)))
        return [
            pltpu.make_async_remote_copy(
                src_ref=ub.at[at], dst_ref=run.at[at],
                send_sem=send_sem if n else lead_sem, recv_sem=arrival(U_NEAR, 0, 0),
                device_id=to, device_id_type=MESH,
            )
            for n, at in enumerate(pieces) if n in which
        ]

    def upper_owner(blocks, kind, target, second=None, passes=None):
        if passes is not None:
            when, greeted, body = passes
            pl.when(when)(lambda: hello(*greeted))
        start_flags()
        places = [(i, s, j) for i, s, j, b in blocks]
        start_loads(FIRST, places)
        start_loads(MATRIX, places)
        flag_copies[0].wait()
        wait_loads(FIRST, places)
        masks = {}
        for i, s, j, b in blocks:
            k = i * SLOTS + s
            masks[k] = pattern[i, j].astype(F32) if kind == U_FAR else None
            value = out[k]
            if kind == U_FAR:
                value = value * masks[k]
                out[k] = value
            ub[0, b] = value.astype(BF16)
        peers = 1 + (second is not None or kind == U_FAR)
        if passes is not None:
            peers = peers + when.astype(jnp.int32)
        pl.semaphore_wait(barrier, peers)
        if second is None:
            for p in range(2):
                send(kind, 0, p, ub, *target)
        else:
            for copy in lead_copies(target, (0, 1, 2)):
                copy.start()
            send(kind, 0, 1, ub, *target)
            lead_copies(target, (0,))[0].wait_send()
            for h in (0, 1):
                hello(r + 1 + h - far_r, c)
        wait_loads(MATRIX, places)
        for i, s, j, b in blocks:
            upper_steps(i * SLOTS + s, b, masks[i * SLOTS + s])
        send(kind, 1, 0, ub, *(second or target))
        send(kind, 1, 1, ub, *target)
        flag_copies[1].wait()
        keep(places)
        if passes is not None:
            @pl.when(when)
            def _():
                own = list(pending)
                pending.clear()
                body()
                drain()
                pending.extend(own)
        if second is not None:
            for copy in lead_copies(target, (1, 2)):
                copy.wait_send()
        drain()

    def pass_diagonal():
        pass_on(D, 0, range(2, rows), (r + 1, c - 1))
        pass_on(D, 1, range(rows), (r + 1, c - 1))

    def near_passer():
        upper = (c + 2 >= far_c) & (c + 2 <= last)
        diag = ~odd & (c + 1 < far_c)
        pl.when(upper)(lambda: hello(r, c + 2))
        pl.when(diag)(lambda: hello(r, c + 1))
        pl.semaphore_wait(barrier, upper.astype(jnp.int32) + diag.astype(jnp.int32))
        sent = {}

        def step(when, name, *what):
            pl.when(when)(lambda: pass_on(*what))
            sent.setdefault(name, (when, []))[1].extend(pending)
            pending.clear()

        if DETOURED[0]:
            step(diag, D, D, 0, DETOURED[0], (r + 1, c + 1))
        step(upper, U_NEAR, U_NEAR, 1, (0,), (r + 1, c + 2))
        if DETOURED[1]:
            step(diag, D, D, 1, DETOURED[1], (r + 1, c + 1))
        for when, own in sent.values():
            pending.extend(own)
            pl.when(when)(drain)
            pending.clear()

    for h in (0, 1):
        pl.when((q == h) & (c == 0))(lambda: diagonal_owner(h, bool(h), False, True, True, bool(h)))
        pl.when((q == h) & (c > 0) & (c < far_c))(lambda: diagonal_owner(h, True, False, True, True))
        pl.when((q == h) & (c >= far_c) & (c < last))(lambda: diagonal_owner(h, True, True, True, False))
        pl.when((q == h) & (c == last))(lambda: diagonal_owner(h, True, True, not h, False))

    near_lower = [(i, OUTER, rows + i, 1 + i, i) for i in range(rows)] + [(0, LEFT, cols - 1, 0, rows - 1)]
    pl.when(q == 2)(lambda: lower_owner(near_lower, L_NEAR, (r - 1, c), (r, c + 1)))

    near_upper = [(rows - 1, RIGHT, 0, 0)] + [(i, OUTER, i, 1 + i) for i in range(rows)]
    pass_lower = (odd & (c >= 3), (r - 1, c - 2), lambda: pass_on(L_NEAR, 1, (*range(1, rows + 1), 0), (r - 1, c - 1)))
    pass_diag = (c == 1, (r, c - 1), pass_diagonal)
    pl.when((q == -1) & (c == 1))(lambda: upper_owner(near_upper, U_NEAR, (r + 1, c), passes=pass_diag))
    pl.when((q == -1) & (c > 1) & (c < far_c))(lambda: upper_owner(near_upper, U_NEAR, (r + 1, c), passes=pass_lower))
    pl.when((q == -1) & (c >= far_c))(
        lambda: upper_owner(near_upper, U_NEAR, (r + 1, c), second=(r, c - 2), passes=pass_lower)
    )
    pl.when((q == 3) & (c + 2 <= last))(near_passer)
    for h in (0, 1):
        far_lower = [(i, OUTER, h * rows + i, i, i) for i in range(rows)]
        far_upper = [(i, OUTER, h * rows + i, i) for i in range(rows)]
        pl.when(q == far_r + h)(lambda: lower_owner(far_lower, L_FAR, (r - far_r, c), (r, c + far_c)))
        pl.when(q == h - far_r)(
            lambda: upper_owner(far_upper, U_FAR, (r + far_r, c))
        )

    out[rows * SLOTS] = jnp.zeros((bs, bs), F32)


def place_kernel(rows, cols, row_devices, bs, blocks, out, sem):
    r, c = lax.axis_index("row"), lax.axis_index("col")
    q = r - (cols // rows) * c
    far = (row_devices // 2) * rows
    copies = []
    for i in range(rows):
        for j in range(cols):
            d = rows * q + i - j
            k = jnp.where(
                d == 0, i * SLOTS + DIAG,
                jnp.where(
                    d == 1, i * SLOTS + LEFT,
                    jnp.where(
                        d == -1, i * SLOTS + RIGHT,
                        jnp.where(
                            (d == rows) | (d == -rows) | (d == far) | (d == -far),
                            i * SLOTS + OUTER, rows * SLOTS,
                        ),
                    ),
                ),
            )
            dst = out.at[pl.ds(i * bs, bs), pl.ds(j * bs, bs)]
            copies.append(pltpu.make_async_copy(blocks.at[k], dst, sem))
    for copy in copies:
        copy.start()
    pltpu.make_async_copy(out, out, sem).wait()


def solution(mesh):
    row_devices, col_devices = mesh.shape["row"], mesh.shape["col"]

    def on_device(matrix, factors, inverse, pattern, dropped):
        rows, cols = pattern.shape
        bs = inverse.shape[1]
        places = rows * SLOTS
        half = lambda *n: pltpu.VMEM(n + (bs, bs), BF16)
        hbm = pl.BlockSpec(memory_space=pl.ANY)
        vmem = pl.BlockSpec(memory_space=pltpu.VMEM)
        blocks = pl.pallas_call(
            functools.partial(sweep_kernel, rows, cols, row_devices, col_devices, bs),
            out_shape=pltpu.VMEM((places + 1, bs, bs), F32),
            in_specs=[hbm] * 5,
            out_specs=vmem,
            scratch_shapes=[
                pltpu.SMEM((rows, cols), jnp.int32), pltpu.SMEM((rows, cols), jnp.int32),
                half(places), half(cols), half(SWEEPS, 2 * rows), half(SWEEPS, 2 * rows),
                half(SWEEPS, rows), half(SWEEPS, rows),
                half(SWEEPS, rows + 1), half(SWEEPS, rows + 1), half(SWEEPS, rows), half(SWEEPS, rows),
                pltpu.VMEM((rows, bs, bs), F32),
                pltpu.SemaphoreType.DMA((2,)),
                pltpu.SemaphoreType.DMA((4,)),
                pltpu.SemaphoreType.DMA,
                pltpu.SemaphoreType.DMA,
                pltpu.SemaphoreType.DMA((SWEEPS * (rows + 7),)),
            ],
            compiler_params=pltpu.CompilerParams(collective_id=0, has_side_effects=True),
            name="sweeps",
        )(pattern, dropped, matrix, factors, inverse)
        return pl.pallas_call(
            functools.partial(place_kernel, rows, cols, row_devices, bs),
            out_shape=jax.ShapeDtypeStruct(factors.shape, F32),
            in_specs=[vmem],
            out_specs=hbm,
            scratch_shapes=[pltpu.SemaphoreType.DMA],
            name="place",
        )(pltpu.with_memory_space_constraint(blocks, pltpu.VMEM))

    placed = (P("row", "col"), P("row", "col"), P("col", None, None), P("row", "col"), P("row", "col"))
    return jax.shard_map(
        on_device, mesh=mesh, in_specs=placed, out_specs=P("row", "col"), check_vma=False
    )
```
